32 devices in a mesh: rows: 8 (over z, y), cols: 4 (over x, core).
Axes of the slice: x: 2, y: 2, z: 4, core: 2. Of those that a mesh axis runs over, the one named last changes fastest.
Arguments:
- gradient: float32 [8192, 29568], P('rows', 'cols'), as said below
- start_block: float32 [29568, 64], P('cols'), may hold values from -0.03125 to 0.03125
- activations: float32 [512, 29568], P('rows', 'cols'), may hold values from -6 to 6
- out_grads: float32 [512, 8192], P('rows', 'cols'), may hold values from -6 to 6
Outputs:
- left_factor: float32 [8192, 64], P('rows')
- right_factor: float32 [29568, 64], P('cols')
- scores: float32 [512], P('rows')
The draws below stay inside these ranges and needn't reach their ends.
Inputs may be any that keep to these rules, and one draw needn't show every extreme that they name: real-valued gradient entries, of order 29568 ** -0.5.
All inputs are finite; a program needn't handle non-finite values.
Results may differ from the reference program's by a relative error of at most 0.00013.
Values sent between devices are 32-bit elements; how exact they have to be, the bound alone decides.
A program may use at most 128 MiB of HBM per device.

```python
import jax
import jax.numpy as jnp
from jax import lax

M = 8192
N = 29568
R = 64
ITERS = 2
TOKENS = 512


def draw_gradient(key, part):
    first, second, third = jax.random.split(jax.random.fold_in(key, 7), 3)
    base = jnp.clip(jax.random.normal(first, (M, N), jnp.float32), -6.0, 6.0)
    upper = 10.0
    rising = 3.0 ** (jnp.arange(M, dtype=jnp.float32) / M)
    row_scale = jnp.exp(jax.random.uniform(second, (M,), jnp.float32) * jnp.log(upper)) * rising
    col_scale = jnp.exp(jax.random.uniform(third, (N,), jnp.float32) * jnp.log(upper))
    return base * row_scale[:, None] * col_scale[None, :] / (40.0 * jnp.sqrt(jnp.float32(N)))


def steps_of(stream_key, dims, pieces, smallest, high):
    level, own = 1.0, jax.random.fold_in(stream_key, 6)
    for axis_at, blocks in pieces:
        heights = jnp.exp(jax.random.uniform(jax.random.fold_in(own, axis_at), (blocks,), jnp.float32, smallest / len(pieces), high / len(pieces)))
        level = level * jnp.repeat(heights, dims[axis_at] // blocks).reshape([-1 if axis == axis_at else 1 for axis in range(len(dims))])
    return level


def scatter_about(key, shape, deviation, limit, cuts=(), held_as=jnp.bfloat16):
    array = deviation * jax.random.normal(key, shape, jnp.float32)
    if cuts:
        array = array * steps_of(key, shape, cuts, -0.22, 0.18)
    return jnp.clip(array, -limit, limit).astype(held_as)


def setup_inputs(seed: int = 0) -> dict:
    key_of = jax.random.split(jax.random.key(seed), 5)
    return {
        "gradient": draw_gradient(jax.random.fold_in(key_of[4], 71), 0),
        "start_block": scatter_about(key_of[1], (N, R), N ** -0.5, 0.03125, ((0, 4),), jnp.float32),
        "activations": scatter_about(key_of[2], (TOKENS, N), 1.0, 6.0, ((0, 8), (1, 4)), jnp.float32),
        "out_grads": scatter_about(key_of[3], (TOKENS, M), 1.0, 6.0, ((0, 8), (1, 4)), jnp.float32),
    }


HIGH = lax.Precision.HIGHEST

def cholqr(block):
    gram = jnp.dot(block.T.astype(jnp.float32), block.astype(jnp.float32), precision=HIGH, preferred_element_type=jnp.float32)
    lower = jnp.linalg.cholesky(gram)
    return lax.linalg.triangular_solve(lower, block, left_side=False, lower=True, transpose_a=True)

def reference(gradient, start_block, activations, out_grads):
    omega = start_block
    for step in range(ITERS):
        ysum = jnp.dot(gradient.astype(jnp.float32), omega.astype(jnp.float32), precision=HIGH, preferred_element_type=jnp.float32)
        left = cholqr(ysum)
        zsum = jnp.dot(gradient.T.astype(jnp.float32), left.astype(jnp.float32), precision=HIGH, preferred_element_type=jnp.float32)
        right = cholqr(zsum)
        omega = right
    core = jnp.dot(left.T.astype(jnp.float32), jnp.dot(gradient.astype(jnp.float32), right.astype(jnp.float32), precision=HIGH, preferred_element_type=jnp.float32).astype(jnp.float32), precision=HIGH, preferred_element_type=jnp.float32)
    token_left = jnp.dot(out_grads.astype(jnp.float32), left.astype(jnp.float32), precision=HIGH, preferred_element_type=jnp.float32)
    token_right = jnp.dot(activations.astype(jnp.float32), right.astype(jnp.float32), precision=HIGH, preferred_element_type=jnp.float32)
    mixed = jnp.dot(token_left.astype(jnp.float32), core.astype(jnp.float32), precision=HIGH, preferred_element_type=jnp.float32)
    scores = jnp.sum(mixed * token_right, axis=1)
    return (left, right, scores)
```

```python
import functools

import jax
import jax.numpy as jnp
from jax import lax
from jax.experimental import pallas as pl
from jax.experimental.pallas import tpu as pltpu
from jax.sharding import PartitionSpec as P

ITERS = 2
HIGH = lax.Precision.HIGHEST
MESH = pl.DeviceIdType.MESH
F32 = jnp.float32
BF16 = jnp.bfloat16
CHUNK = 256
TILE = 64
SEGMENTS = 7
NT = (((1,), (1,)), ((), ()))
NN = (((1,), (0,)), ((), ()))


def dot(a, b, dims, precision=None):
    return lax.dot_general(a, b, dims, precision=precision, preferred_element_type=F32)


def split(x):
    hi = x.astype(BF16)
    return hi, (x - hi.astype(F32)).astype(BF16)


def chol_inverse(gram):
    n = gram.shape[0]
    sub = lax.broadcasted_iota(jnp.int32, (n, 2 * n), 0)
    lane = lax.broadcasted_iota(jnp.int32, (n, 2 * n), 1)
    eye = (lax.broadcasted_iota(jnp.int32, (n, n), 0) == lax.broadcasted_iota(jnp.int32, (n, n), 1)).astype(F32)
    w = jnp.concatenate([gram, eye], axis=1)
    for k in range(n):
        row = w[k : k + 1, :]
        scaled = row * (1.0 / row[:, k : k + 1])
        w = w - jnp.where(sub > k, w[:, k : k + 1], 0.0) * scaled
    diag = jnp.sum(jnp.where(sub == lane, w, 0.0), axis=1, keepdims=True)
    w = w * (1.0 / jnp.sqrt(diag))
    return w[:, :n], w[:, n:]


def pack(gram):
    half = gram.shape[0] // 2
    return jnp.concatenate([gram[:half], gram[half:]], axis=1)


def unpack(packed):
    n = packed.shape[1] // 2
    return jnp.concatenate([packed[:, :n], packed[:, n:]], axis=0)


def kernel(
    rows, cols, g_ref, w0_ref, left_ref, right_ref, core_ref,
    ghi, glo, fbuf, wcat, lcat, acc, ypart, yrecv, yfull, zpart, zpair, zgroup, zfull, gacc, grow, gcol,
    load_sem, ys_s, ys_r, ya_s, ya_r, gr_s, gr_r, gc_s, gc_r, p_s, p_r, q_s, q_r, a_s, a_r, b_s, b_r,
):
    r, c = lax.axis_index("rows"), lax.axis_index("cols")
    rank, wide = zfull.shape
    depth, n = g_ref.shape
    groups = rows // 2
    y, q = lax.rem(r, 2), lax.div(r, 2)
    half, eighth, quarter = rank // 2, rank // rows, rank // cols
    chunks = wide // CHUNK

    def load(t, slot):
        return pltpu.make_async_copy(
            g_ref.at[pl.ds(pl.multiple_of(t * TILE, TILE), TILE), :], fbuf.at[slot], load_sem.at[slot]
        )

    load(0, 0).start()

    barrier = pltpu.get_barrier_semaphore()
    for d in range(1, rows):
        pl.semaphore_signal(barrier, inc=1, device_id=(lax.rem(r + d, rows), c), device_id_type=MESH)
    for d in range(1, cols):
        pl.semaphore_signal(barrier, inc=1, device_id=(r, lax.rem(c + d, cols)), device_id_type=MESH)

    def put_factor(block, off):
        hi, lo = split(block)
        wcat[:rank, pl.ds(off, CHUNK)] = hi
        wcat[rank:, pl.ds(off, CHUNK)] = lo

    @pl.loop(0, chunks)
    def _(k):
        off = pl.multiple_of(k * CHUNK, CHUNK)
        put_factor(w0_ref[:, pl.ds(off, CHUNK)], off)

    ghi[:, wide - CHUNK :] = jnp.zeros((depth, CHUNK), BF16)
    glo[:, wide - CHUNK :] = jnp.zeros((depth, CHUNK), BF16)
    tiles = depth // TILE

    @pl.loop(0, tiles)
    def _(t):
        slot = lax.rem(t, 2)
        load(t, slot).wait()

        @pl.when(t + 1 < tiles)
        def _():
            load(t + 1, 1 - slot).start()

        hi, lo = split(fbuf[slot])
        at = pl.ds(pl.multiple_of(t * TILE, TILE), TILE)
        ghi[at, :n] = hi
        glo[at, :n] = lo

    pl.semaphore_wait(barrier, rows + cols - 2)

    def copy(src, dst, ssem, rsem, dev):
        cp = pltpu.make_async_remote_copy(
            src_ref=src, dst_ref=dst, send_sem=ssem, recv_sem=rsem, device_id=dev, device_id_type=MESH
        )
        cp.start()
        return cp

    def exchange(slots, me, count, ssem, rsem, device):
        cps = []
        for d in range(1, count):
            cps.append(copy(slots.at[me], slots.at[me], ssem.at[d - 1], rsem.at[d - 1], device(lax.rem(me + d, count))))
        for cp in cps:
            cp.wait()
        total = slots[0]
        for i in range(1, count):
            total = total + slots[i]
        return unpack(total)

    def rows_at(start, size):
        return pl.ds(pl.multiple_of(start, 8), size)

    bounds = [(chunks * s) // SEGMENTS for s in range(SEGMENTS + 1)]

    for step in range(ITERS):
        last = step == ITERS - 1
        acc[...] = jnp.zeros_like(acc)

        @pl.loop(0, chunks)
        def _(k):
            at = pl.ds(pl.multiple_of(k * CHUNK, CHUNK), CHUNK)
            w = wcat[:, at]
            acc[...] += dot(ghi[:, at], w, NT) + dot(glo[:, at], w, NT)

        for i in range(0, depth, 128):
            turned = acc[i : i + 128, :].T
            ypart[:, i : i + 128] = turned[:rank] + turned[rank:]
        cps = []
        for d in range(1, cols):
            p = lax.rem(c + d, cols)
            cps.append(copy(ypart.at[rows_at(p * quarter, quarter)], yrecv.at[d - 1], ys_s.at[d - 1], ys_r.at[d - 1], (r, p)))
        for cp in cps:
            cp.wait()
        own = rows_at(c * quarter, quarter)
        total = ypart[own, :]
        for d in range(1, cols):
            total = total + yrecv[d - 1]
        yfull[own, :] = total
        cps = []
        for d in range(1, cols):
            p = lax.rem(c + d, cols)
            cps.append(copy(yfull.at[own], yfull.at[own], ya_s.at[d - 1], ya_r.at[d - 1], (r, p)))
        for cp in cps:
            cp.wait()
        grow[r] = pack(dot(yfull[...], yfull[...], NT, HIGH))
        gram = exchange(grow, r, rows, gr_s, gr_r, lambda p: (p, c))
        _, inverse = chol_inverse(gram)
        left = dot(inverse, yfull[...], NN, HIGH)
        if last:
            left_ref[...] = left
        hi, lo = split(left)
        lcat[:rank, :] = hi
        lcat[rank:, :] = lo
        gacc[...] = jnp.zeros_like(gacc)
        flight = {}
        sends = []
        pair = (r + 1 - 2 * y, c)

        def start(key, cp):
            flight.setdefault(key, []).append(cp)
            sends.append(cp)

        def arrived(key):
            for cp in flight[key]:
                cp.wait_recv()

        def seg_at(s):
            return pl.ds(bounds[s] * CHUNK, (bounds[s + 1] - bounds[s]) * CHUNK)

        def stage0(s):
            @pl.loop(bounds[s], bounds[s + 1])
            def _(k):
                at = pl.ds(pl.multiple_of(k * CHUNK, CHUNK), CHUNK)
                part = dot(lcat[...], ghi[:, at], NN) + dot(lcat[...], glo[:, at], NN)
                zpart[:, at] = part[:rank] + part[rank:]

            other = rows_at((1 - y) * half, half)
            start(("p", s), copy(zpart.at[other, seg_at(s)], zpair.at[:, seg_at(s)], p_s.at[s], p_r.at[s], pair))

        def stage1(s):
            arrived(("p", s))
            at = seg_at(s)
            zpair[:, at] = zpair[:, at] + zpart[rows_at(y * half, half), at]
            for d in range(1, groups):
                p = lax.rem(q + d, groups)
                start(
                    ("q", s),
                    copy(
                        zpair.at[rows_at(p * eighth, eighth), at], zgroup.at[d - 1, :, at],
                        q_s.at[s, d - 1], q_r.at[s, d - 1], (2 * p + y, c),
                    ),
                )

        mine = rows_at(y * half + q * eighth, eighth)

        def stage2(s):
            arrived(("q", s))
            at = seg_at(s)
            total = zpair[rows_at(q * eighth, eighth), at]
            for d in range(1, groups):
                total = total + zgroup[d - 1, :, at]
            zfull[mine, at] = total
            for d in range(1, groups):
                p = lax.rem(q + d, groups)
                start(
                    ("a", s),
                    copy(zfull.at[mine, at], zfull.at[mine, at], a_s.at[s, d - 1], a_r.at[s, d - 1], (2 * p + y, c)),
                )

        def stage3(s):
            arrived(("a", s))
            at = seg_at(s)
            kept = rows_at(y * half, half)
            start(("b", s), copy(zfull.at[kept, at], zfull.at[kept, at], b_s.at[s], b_r.at[s], pair))

        def stage4(s):
            arrived(("b", s))
            block = zfull[:, seg_at(s)]
            gacc[...] += dot(block, block, NT, HIGH)

        stages = (stage0, stage1, stage2, stage3, stage4)
        for tick in range(SEGMENTS + len(stages) - 1):
            for i, stage in enumerate(stages):
                if 0 <= tick - i < SEGMENTS:
                    stage(tick - i)
        for cp in sends:
            cp.wait_send()
        gcol[c] = pack(gacc[...])
        gram = exchange(gcol, c, cols, gc_s, gc_r, lambda p: (r, p))
        upper, inverse = chol_inverse(gram)
        if last:
            core_ref[...] = upper

        @pl.loop(0, chunks)
        def _(k):
            off = pl.multiple_of(k * CHUNK, CHUNK)
            block = dot(inverse, zfull[:, pl.ds(off, CHUNK)], NN, HIGH)
            if last:
                right_ref[:, pl.ds(off, CHUNK)] = block
            else:
                put_factor(block, off)


def iterate(gradient, start, rows, cols):
    depth, n = gradient.shape
    rank, wide = start.shape
    dma = pltpu.SemaphoreType.DMA
    groups = rows // 2
    vmem = pl.BlockSpec(memory_space=pltpu.VMEM)
    return pl.pallas_call(
        functools.partial(kernel, rows, cols),
        out_shape=(
            jax.ShapeDtypeStruct((rank, depth), F32),
            jax.ShapeDtypeStruct((rank, wide), F32),
            jax.ShapeDtypeStruct((rank, rank), F32),
        ),
        in_specs=[pl.BlockSpec(memory_space=pl.ANY), vmem],
        out_specs=(vmem, vmem, vmem),
        scratch_shapes=[
            pltpu.VMEM((depth, wide), BF16),
            pltpu.VMEM((depth, wide), BF16),
            pltpu.VMEM((2, TILE, n), F32),
            pltpu.VMEM((2 * rank, wide), BF16),
            pltpu.VMEM((2 * rank, depth), BF16),
            pltpu.VMEM((depth, 2 * rank), F32),
            pltpu.VMEM((rank, depth), F32),
            pltpu.VMEM((cols - 1, rank // cols, depth), F32),
            pltpu.VMEM((rank, depth), F32),
            pltpu.VMEM((rank, wide), F32),
            pltpu.VMEM((rank // 2, wide), F32),
            pltpu.VMEM((groups - 1, rank // rows, wide), F32),
            pltpu.VMEM((rank, wide), F32),
            pltpu.VMEM((rank, rank), F32),
            pltpu.VMEM((rows, rank // 2, 2 * rank), F32),
            pltpu.VMEM((cols, rank // 2, 2 * rank), F32),
            dma((2,)),
            dma((cols - 1,)), dma((cols - 1,)), dma((cols - 1,)), dma((cols - 1,)),
            dma((rows - 1,)), dma((rows - 1,)), dma((cols - 1,)), dma((cols - 1,)),
            dma((SEGMENTS,)), dma((SEGMENTS,)),
            dma((SEGMENTS, groups - 1)), dma((SEGMENTS, groups - 1)),
            dma((SEGMENTS, groups - 1)), dma((SEGMENTS, groups - 1)),
            dma((SEGMENTS,)), dma((SEGMENTS,)),
        ],
        compiler_params=pltpu.CompilerParams(
            collective_id=0, has_side_effects=True, vmem_limit_bytes=60 * 1024 * 1024
        ),
        cost_estimate=pl.CostEstimate(flops=16 * depth * n * rank, bytes_accessed=4 * depth * n, transcendentals=0),
    )(gradient, start)


def factor_with(block, gram):
    lower = jnp.linalg.cholesky(gram)
    return (
        lax.linalg.triangular_solve(lower, block, left_side=False, lower=True, transpose_a=True),
        lower,
    )


def full_dot(a, b):
    return jnp.dot(a, b, precision=HIGH, preferred_element_type=F32)


def iterate_plain(gradient, start_block):
    omega = start_block
    for step in range(ITERS):
        ysum = lax.psum(full_dot(gradient, omega), "cols")
        left, lower_y = factor_with(ysum, lax.psum(full_dot(ysum.T, ysum), "rows"))
        zsum = lax.psum(full_dot(gradient.T, left), "rows")
        right, lower_z = factor_with(zsum, lax.psum(full_dot(zsum.T, zsum), "cols"))
        omega = right
    return left, right, lower_z


def fits(rows, cols, depth, n, rank):
    wide = -(-n // CHUNK) * CHUNK
    held = 4 * depth * wide + 4 * rank * wide * 6
    return (
        rows % 2 == 0 and rows > 2 and cols > 1 and rank % (8 * rows) == 0 and rank % (8 * cols) == 0
        and 2 * rank == 128 and depth % 128 == 0 and wide // CHUNK >= SEGMENTS and held < 50 * 1024 * 1024
    )


def per_device(rows, cols, gradient, start_block, activations, out_grads):
    depth, n = gradient.shape
    rank = start_block.shape[1]
    grad_cols = out_grads.shape[1]
    if fits(rows, cols, depth, n, rank):
        wide = -(-n // CHUNK) * CHUNK
        start = jnp.pad(start_block.T, ((0, 0), (0, wide - n)))
        left, right, upper = iterate(gradient, start, rows, cols)
        left, right, lower_z = left.T, right[:, :n].T, upper.T
    else:
        left, right, lower_z = iterate_plain(gradient, start_block)
    whole_rows = lax.all_gather(left, "rows", axis=0, tiled=True)
    left_cols = lax.dynamic_slice_in_dim(whole_rows, lax.axis_index("cols") * grad_cols, grad_cols, 0)
    token_left, token_right = lax.psum((full_dot(out_grads, left_cols), full_dot(activations, right)), "cols")
    scores = jnp.sum(full_dot(token_left, lower_z) * token_right, axis=1)
    return (left, right, scores)


def solution(mesh):
    placed = (P("rows", "cols"), P("cols", None), P("rows", "cols"), P("rows", "cols"))
    return jax.shard_map(
        functools.partial(per_device, mesh.shape["rows"], mesh.shape["cols"]),
        mesh=mesh,
        in_specs=placed,
        out_specs=(P("rows", None), P("cols", None), P("rows")),
        check_vma=False,
    )
```

```python
import functools

import jax
import jax.numpy as jnp
from jax import lax
from jax.experimental import pallas as pl
from jax.experimental.pallas import tpu as pltpu
from jax.sharding import PartitionSpec as P

ITERS = 2
HIGH = lax.Precision.HIGHEST
MESH = pl.DeviceIdType.MESH
F32 = jnp.float32
BF16 = jnp.bfloat16
CHUNK = 256
SLOTS = 4
SEGMENTS = 7
NT = (((1,), (1,)), ((), ()))
NN = (((1,), (0,)), ((), ()))


def dot(a, b, dims, precision=None):
    return lax.dot_general(a, b, dims, precision=precision, preferred_element_type=F32)


def split(x):
    hi = x.astype(BF16)
    return hi, (x - hi.astype(F32)).astype(BF16)


def chol_inverse(gram):
    n = gram.shape[0]
    sub = lax.broadcasted_iota(jnp.int32, (n, 2 * n), 0)
    lane = lax.broadcasted_iota(jnp.int32, (n, 2 * n), 1)
    eye = (lax.broadcasted_iota(jnp.int32, (n, n), 0) == lax.broadcasted_iota(jnp.int32, (n, n), 1)).astype(F32)
    w = jnp.concatenate([gram, eye], axis=1)
    for k in range(n):
        row = w[k : k + 1, :]
        scaled = row * (1.0 / row[:, k : k + 1])
        w = w - jnp.where(sub > k, w[:, k : k + 1], 0.0) * scaled
    diag = jnp.sum(jnp.where(sub == lane, w, 0.0), axis=1, keepdims=True)
    w = w * (1.0 / jnp.sqrt(diag))
    return w[:, :n], w[:, n:]


def pack(gram):
    half = gram.shape[0] // 2
    return jnp.concatenate([gram[:half], gram[half:]], axis=1)


def unpack(packed):
    n = packed.shape[1] // 2
    return jnp.concatenate([packed[:, :n], packed[:, n:]], axis=0)


def kernel(
    rows, cols, g_ref, w0_ref, act_ref, og_ref, left_ref, right_ref, score_ref,
    ghi, glo, fbuf, ftail, wcat, lcat, acc, ypart, yrecv, yfull, zpart, zpair, zgroup, zfull, gacc, grow, gcol, lsel, tok,
    load_sem, tail_sem, ys_s, ys_r, ya_s, ya_r, gr_s, gr_r, gc_s, gc_r, p_s, p_r, q_s, q_r, a_s, a_r, b_s, b_r,
    l_s, l_r, m_s, m_r, t_s, t_r,
):
    r, c = lax.axis_index("rows"), lax.axis_index("cols")
    rank, wide = zfull.shape
    n, depth = g_ref.shape
    groups = rows // 2
    y, q = lax.rem(r, 2), lax.div(r, 2)
    half, eighth, quarter = rank // 2, rank // rows, rank // cols
    chunks, full = wide // CHUNK, n // CHUNK
    cut, rest = full * CHUNK, n - full * CHUNK

    def load(k):
        slot = lax.rem(k, SLOTS)
        at = pl.ds(pl.multiple_of(k * CHUNK, CHUNK), CHUNK)
        return pltpu.make_async_copy(g_ref.at[at, :], fbuf.at[slot], load_sem.at[slot])

    for k in range(SLOTS):
        load(k).start()
    if rest:
        load_tail = pltpu.make_async_copy(g_ref.at[cut:n, :], ftail, tail_sem.at[0])
        load_tail.start()

    barrier = pltpu.get_barrier_semaphore()
    for d in range(1, rows):
        pl.semaphore_signal(barrier, inc=1, device_id=(lax.rem(r + d, rows), c), device_id_type=MESH)
    for d in range(1, cols):
        pl.semaphore_signal(barrier, inc=1, device_id=(r, lax.rem(c + d, cols)), device_id_type=MESH)

    def put_factor(block, off):
        hi, lo = split(block)
        wcat[:rank, pl.ds(off, CHUNK)] = hi
        wcat[rank:, pl.ds(off, CHUNK)] = lo

    def times(k):
        at = pl.ds(pl.multiple_of(k * CHUNK, CHUNK), CHUNK)
        w = wcat[:, at]
        acc[...] += dot(w, ghi[at, :], NN) + dot(w, glo[at, :], NN)

    acc[...] = jnp.zeros_like(acc)

    @pl.loop(0, full)
    def _(k):
        slot = lax.rem(k, SLOTS)
        off = pl.multiple_of(k * CHUNK, CHUNK)
        put_factor(w0_ref[:, pl.ds(off, CHUNK)], off)
        load(k).wait()
        hi, lo = split(fbuf[slot])
        ghi[pl.ds(off, CHUNK), :] = hi
        glo[pl.ds(off, CHUNK), :] = lo

        @pl.when(k + SLOTS < full)
        def _():
            load(k + SLOTS).start()

        times(k)

    if rest:
        wcat[:, cut:] = jnp.zeros((2 * rank, CHUNK), BF16)
        ghi[cut:, :] = jnp.zeros((CHUNK, depth), BF16)
        glo[cut:, :] = jnp.zeros((CHUNK, depth), BF16)
        hi, lo = split(w0_ref[:, cut:n])
        wcat[:rank, cut:n] = hi
        wcat[rank:, cut:n] = lo
        load_tail.wait()
        hi, lo = split(ftail[...])
        ghi[cut:n, :] = hi
        glo[cut:n, :] = lo
        times(full)

    pl.semaphore_wait(barrier, rows + cols - 2)

    def copy(src, dst, ssem, rsem, dev):
        cp = pltpu.make_async_remote_copy(
            src_ref=src, dst_ref=dst, send_sem=ssem, recv_sem=rsem, device_id=dev, device_id_type=MESH
        )
        cp.start()
        return cp

    def exchange(slots, me, count, ssem, rsem, device):
        cps = []
        for d in range(1, count):
            cps.append(copy(slots.at[me], slots.at[me], ssem.at[d - 1], rsem.at[d - 1], device(lax.rem(me + d, count))))
        for cp in cps:
            cp.wait()
        total = slots[0]
        for i in range(1, count):
            total = total + slots[i]
        return total

    def rows_at(start, size):
        return pl.ds(pl.multiple_of(start, 8), size)

    bounds = [(chunks * s) // SEGMENTS for s in range(SEGMENTS + 1)]

    for step in range(ITERS):
        last = step == ITERS - 1
        if step:
            acc[...] = jnp.zeros_like(acc)
            pl.loop(0, chunks)(times)
        ypart[...] = acc[:rank, :] + acc[rank:, :]
        cps = []
        for d in range(1, cols):
            p = lax.rem(c + d, cols)
            cps.append(copy(ypart.at[rows_at(p * quarter, quarter)], yrecv.at[d - 1], ys_s.at[d - 1], ys_r.at[d - 1], (r, p)))
        for cp in cps:
            cp.wait()
        own = rows_at(c * quarter, quarter)
        total = ypart[own, :]
        for d in range(1, cols):
            total = total + yrecv[d - 1]
        yfull[own, :] = total
        cps = []
        for d in range(1, cols):
            p = lax.rem(c + d, cols)
            cps.append(copy(yfull.at[own], yfull.at[own], ya_s.at[d - 1], ya_r.at[d - 1], (r, p)))
        for cp in cps:
            cp.wait()
        grow[r] = pack(dot(yfull[...], yfull[...], NT, HIGH))
        gram = unpack(exchange(grow, r, rows, gr_s, gr_r, lambda p: (p, c)))
        _, inverse = chol_inverse(gram)
        left = dot(inverse, yfull[...], NN, HIGH)
        if last:
            left_ref[...] = left

            @pl.when(q == c)
            def _():
                lsel[y] = left
        hi, lo = split(left)
        lcat[:rank, :] = hi
        lcat[rank:, :] = lo
        gacc[...] = jnp.zeros_like(gacc)
        flight = {}
        sends = []
        pair = (r + 1 - 2 * y, c)

        def start(key, cp):
            flight.setdefault(key, []).append(cp)
            sends.append(cp)

        def arrived(key):
            for cp in flight[key]:
                cp.wait_recv()

        def seg_at(s):
            return pl.ds(bounds[s] * CHUNK, (bounds[s + 1] - bounds[s]) * CHUNK)

        def stage0(s):
            @pl.loop(bounds[s], bounds[s + 1])
            def _(k):
                at = pl.ds(pl.multiple_of(k * CHUNK, CHUNK), CHUNK)
                part = (dot(ghi[at, :], lcat[...], NT) + dot(glo[at, :], lcat[...], NT)).T
                zpart[:, at] = part[:rank] + part[rank:]

            other = rows_at((1 - y) * half, half)
            start(("p", s), copy(zpart.at[other, seg_at(s)], zpair.at[:, seg_at(s)], p_s.at[s], p_r.at[s], pair))

        def stage1(s):
            arrived(("p", s))
            at = seg_at(s)
            zpair[:, at] = zpair[:, at] + zpart[rows_at(y * half, half), at]
            for d in range(1, groups):
                p = lax.rem(q + d, groups)
                start(
                    ("q", s),
                    copy(
                        zpair.at[rows_at(p * eighth, eighth), at], zgroup.at[d - 1, :, at],
                        q_s.at[s, d - 1], q_r.at[s, d - 1], (2 * p + y, c),
                    ),
                )

        mine = rows_at(y * half + q * eighth, eighth)

        def stage2(s):
            arrived(("q", s))
            at = seg_at(s)
            total = zpair[rows_at(q * eighth, eighth), at]
            for d in range(1, groups):
                total = total + zgroup[d - 1, :, at]
            zfull[mine, at] = total
            for d in range(1, groups):
                p = lax.rem(q + d, groups)
                start(
                    ("a", s),
                    copy(zfull.at[mine, at], zfull.at[mine, at], a_s.at[s, d - 1], a_r.at[s, d - 1], (2 * p + y, c)),
                )

        def stage3(s):
            arrived(("a", s))
            at = seg_at(s)
            kept = rows_at(y * half, half)
            start(("b", s), copy(zfull.at[kept, at], zfull.at[kept, at], b_s.at[s], b_r.at[s], pair))

        def stage4(s):
            arrived(("b", s))
            block = zfull[:, seg_at(s)]
            gacc[...] += dot(block, block, NT, HIGH)

        stages = (stage0, stage1, stage2, stage3, stage4)
        for tick in range(SEGMENTS + len(stages) - 1):
            for i, stage in enumerate(stages):
                if 0 <= tick - i < SEGMENTS:
                    stage(tick - i)
        for cp in sends:
            cp.wait_send()
        if last:
            def spread(d):
                return pltpu.make_async_remote_copy(
                    src_ref=left_ref, dst_ref=lsel.at[y], send_sem=l_s.at[d - 1], recv_sem=l_r.at[0],
                    device_id=(2 * lax.rem(q + d, groups) + y, c), device_id_type=MESH,
                )

            @pl.when(q == c)
            def _():
                for d in range(1, groups):
                    spread(d).start()
        gcol[c] = pack(gacc[...])
        gram = unpack(exchange(gcol, c, cols, gc_s, gc_r, lambda p: (r, p)))
        upper, inverse = chol_inverse(gram)
        if not last:

            @pl.loop(0, chunks)
            def _(k):
                off = pl.multiple_of(k * CHUNK, CHUNK)
                put_factor(dot(inverse, zfull[:, pl.ds(off, CHUNK)], NN, HIGH), off)

    @pl.when(q != c)
    def _():
        spread(1).wait_recv()

    swap = copy(lsel.at[y], lsel.at[y], m_s.at[0], m_r.at[0], pair)
    gacc[...] = jnp.zeros_like(gacc)

    @pl.loop(0, full)
    def _(k):
        at = pl.ds(pl.multiple_of(k * CHUNK, CHUNK), CHUNK)
        block = dot(inverse, zfull[:, at], NN, HIGH)
        right_ref[:, at] = block
        gacc[...] += dot(act_ref[:, at], block, NT, HIGH)

    if rest:
        block = dot(inverse, zfull[:, cut:], NN, HIGH)[:, :rest]
        right_ref[:, cut:n] = block
        gacc[...] += dot(act_ref[:, cut:n], block, NT, HIGH)
    swap.wait()

    @pl.when(q == c)
    def _():
        for d in range(1, groups):
            spread(d).wait_send()

    token_left = dot(og_ref[:, :depth], lsel[0], NT, HIGH) + dot(og_ref[:, depth:], lsel[1], NT, HIGH)
    tok[c] = jnp.concatenate([token_left, gacc[...]], axis=1)
    tokens = exchange(tok, c, cols, t_s, t_r, lambda p: (r, p))
    mixed = dot(tokens[:, :rank], upper, NT, HIGH)
    score_ref[...] = dot(jnp.ones((8, rank), F32), mixed * tokens[:, rank:], NT, HIGH)


def iterate(gradient, start, activations, out_grads, rows, cols):
    n, depth = gradient.shape
    rank = start.shape[0]
    tokens = activations.shape[0]
    wide = -(-n // CHUNK) * CHUNK
    dma = pltpu.SemaphoreType.DMA
    groups = rows // 2
    vmem = pl.BlockSpec(memory_space=pltpu.VMEM)
    return pl.pallas_call(
        functools.partial(kernel, rows, cols),
        out_shape=(
            jax.ShapeDtypeStruct((rank, depth), F32),
            jax.ShapeDtypeStruct((rank, n), F32),
            jax.ShapeDtypeStruct((8, tokens), F32),
        ),
        in_specs=[pl.BlockSpec(memory_space=pl.ANY), vmem, vmem, vmem],
        out_specs=(vmem, vmem, vmem),
        scratch_shapes=[
            pltpu.VMEM((wide, depth), BF16),
            pltpu.VMEM((wide, depth), BF16),
            pltpu.VMEM((SLOTS, CHUNK, depth), F32),
            pltpu.VMEM((n % CHUNK or 8, depth), F32),
            pltpu.VMEM((2 * rank, wide), BF16),
            pltpu.VMEM((2 * rank, depth), BF16),
            pltpu.VMEM((2 * rank, depth), F32),
            pltpu.VMEM((rank, depth), F32),
            pltpu.VMEM((cols - 1, rank // cols, depth), F32),
            pltpu.VMEM((rank, depth), F32),
            pltpu.VMEM((rank, wide), F32),
            pltpu.VMEM((rank // 2, wide), F32),
            pltpu.VMEM((groups - 1, rank // rows, wide), F32),
            pltpu.VMEM((rank, wide), F32),
            pltpu.VMEM((rank, rank), F32),
            pltpu.VMEM((rows, rank // 2, 2 * rank), F32),
            pltpu.VMEM((cols, rank // 2, 2 * rank), F32),
            pltpu.VMEM((2, rank, depth), F32),
            pltpu.VMEM((cols, tokens, 2 * rank), F32),
            dma((SLOTS,)), dma((1,)),
            dma((cols - 1,)), dma((cols - 1,)), dma((cols - 1,)), dma((cols - 1,)),
            dma((rows - 1,)), dma((rows - 1,)), dma((cols - 1,)), dma((cols - 1,)),
            dma((SEGMENTS,)), dma((SEGMENTS,)),
            dma((SEGMENTS, groups - 1)), dma((SEGMENTS, groups - 1)),
            dma((SEGMENTS, groups - 1)), dma((SEGMENTS, groups - 1)),
            dma((SEGMENTS,)), dma((SEGMENTS,)),
            dma((groups - 1,)), dma((1,)), dma((1,)), dma((1,)), dma((cols - 1,)), dma((cols - 1,)),
        ],
        compiler_params=pltpu.CompilerParams(
            collective_id=0, has_side_effects=True, vmem_limit_bytes=63 * 1024 * 1024
        ),
        cost_estimate=pl.CostEstimate(flops=16 * depth * n * rank, bytes_accessed=4 * depth * n, transcendentals=0),
    )(gradient, start, activations, out_grads)


def factor_with(block, gram):
    lower = jnp.linalg.cholesky(gram)
    return (
        lax.linalg.triangular_solve(lower, block, left_side=False, lower=True, transpose_a=True),
        lower,
    )


def full_dot(a, b):
    return jnp.dot(a, b, precision=HIGH, preferred_element_type=F32)


def iterate_plain(gradient, start_block):
    omega = start_block
    for step in range(ITERS):
        ysum = lax.psum(full_dot(gradient, omega), "cols")
        left, lower_y = factor_with(ysum, lax.psum(full_dot(ysum.T, ysum), "rows"))
        zsum = lax.psum(full_dot(gradient.T, left), "rows")
        right, lower_z = factor_with(zsum, lax.psum(full_dot(zsum.T, zsum), "cols"))
        omega = right
    return left, right, lower_z


def fits(rows, cols, depth, n, rank, tokens, grad_cols):
    wide = -(-n // CHUNK) * CHUNK
    held = 4 * depth * wide + 4 * rank * wide * 7
    return (
        rows == 2 * cols and cols > 1 and rank % (8 * rows) == 0 and 2 * rank == 128 and depth % 128 == 0
        and n % 16 == 0 and n // CHUNK >= max(SEGMENTS, SLOTS) and held < 50 * 1024 * 1024
        and grad_cols == 2 * depth and tokens % 8 == 0 and tokens <= 128
    )


def per_device(rows, cols, gradient, start_block, activations, out_grads):
    depth, n = gradient.shape
    rank = start_block.shape[1]
    tokens, grad_cols = out_grads.shape
    if fits(rows, cols, depth, n, rank, tokens, grad_cols):
        left, right, scores = iterate(gradient.T, start_block.T, activations, out_grads, rows, cols)
        return left.T, right.T, scores[0]
    left, right, lower_z = iterate_plain(gradient, start_block)
    whole_rows = lax.all_gather(left, "rows", axis=0, tiled=True)
    left_cols = lax.dynamic_slice_in_dim(whole_rows, lax.axis_index("cols") * grad_cols, grad_cols, 0)
    token_left, token_right = lax.psum((full_dot(out_grads, left_cols), full_dot(activations, right)), "cols")
    scores = jnp.sum(full_dot(token_left, lower_z) * token_right, axis=1)
    return (left, right, scores)


def solution(mesh):
    placed = (P("rows", "cols"), P("cols", None), P("rows", "cols"), P("rows", "cols"))
    return jax.shard_map(
        functools.partial(per_device, mesh.shape["rows"], mesh.shape["cols"]),
        mesh=mesh,
        in_specs=placed,
        out_specs=(P("rows", None), P("cols", None), P("rows")),
        check_vma=False,
    )
```

```python
import functools

import jax
import jax.numpy as jnp
from jax import lax
from jax.experimental import pallas as pl
from jax.experimental.pallas import tpu as pltpu
from jax.sharding import PartitionSpec as P

ITERS = 2
HIGH = lax.Precision.HIGHEST
MESH = pl.DeviceIdType.MESH
F32 = jnp.float32
BF16 = jnp.bfloat16
CHUNK = 256
SLOTS = 4
SEGMENTS = 7
NT = (((1,), (1,)), ((), ()))
NN = (((1,), (0,)), ((), ()))


def dot(a, b, dims, precision=None):
    return lax.dot_general(a, b, dims, precision=precision, preferred_element_type=F32)


def split(x):
    hi = x.astype(BF16)
    return hi, (x - hi.astype(F32)).astype(BF16)


def chol_inverse(gram):
    n = gram.shape[0]
    sub = lax.broadcasted_iota(jnp.int32, (n, 2 * n), 0)
    lane = lax.broadcasted_iota(jnp.int32, (n, 2 * n), 1)
    eye = (lax.broadcasted_iota(jnp.int32, (n, n), 0) == lax.broadcasted_iota(jnp.int32, (n, n), 1)).astype(F32)
    w = jnp.concatenate([gram, eye], axis=1)
    for k in range(0, n, 2):
        row0, row1 = w[k : k + 1, :], w[k + 1 : k + 2, :]
        col0, col1 = w[:, k : k + 1], w[:, k + 1 : k + 2]
        inv0 = 1.0 / row0[:, k : k + 1]
        scaled0 = row0 * inv0
        below = row1[:, k : k + 1]
        across = row0[:, k + 1 : k + 2] * inv0
        inv1 = 1.0 / (row1[:, k + 1 : k + 2] - below * across)
        scaled1 = (row1 - below * scaled0) * inv1
        w = w - jnp.where(sub > k, col0, 0.0) * scaled0 - jnp.where(sub > k + 1, col1 - col0 * across, 0.0) * scaled1
    diag = jnp.sum(jnp.where(sub == lane, w, 0.0), axis=1, keepdims=True)
    w = w * (1.0 / jnp.sqrt(diag))
    return w[:, :n], w[:, n:]


def pack(gram):
    half = gram.shape[0] // 2
    return jnp.concatenate([gram[:half], gram[half:]], axis=1)


def unpack(packed):
    n = packed.shape[1] // 2
    return jnp.concatenate([packed[:, :n], packed[:, n:]], axis=0)


def kernel(
    rows, cols, g_ref, w0_ref, act_ref, og_ref, left_ref, right_ref, score_ref,
    ghi, glo, fbuf, ftail, wcat, lcat, acc, ypart, yrecv, yfull, zpart, zpair, zgroup, zfull, gacc, grow, gcol, lsel, tok,
    load_sem, tail_sem, ys_s, ys_r, ya_s, ya_r, gr_s, gr_r, gc_s, gc_r, p_s, p_r, q_s, q_r, a_s, a_r, b_s, b_r,
    l_s, l_r, m_s, m_r, t_s, t_r,
):
    r, c = lax.axis_index("rows"), lax.axis_index("cols")
    rank, wide = zfull.shape
    n, depth = g_ref.shape
    groups = rows // 2
    y, q = lax.rem(r, 2), lax.div(r, 2)
    half, eighth, quarter = rank // 2, rank // rows, rank // cols
    chunks, full = wide // CHUNK, n // CHUNK
    cut, rest = full * CHUNK, n - full * CHUNK

    def load(k):
        slot = lax.rem(k, SLOTS)
        at = pl.ds(pl.multiple_of(k * CHUNK, CHUNK), CHUNK)
        return pltpu.make_async_copy(g_ref.at[at, :], fbuf.at[slot], load_sem.at[slot])

    for k in range(SLOTS):
        load(k).start()
    if rest:
        load_tail = pltpu.make_async_copy(g_ref.at[cut:n, :], ftail, tail_sem.at[0])
        load_tail.start()

    barrier = pltpu.get_barrier_semaphore()
    for d in range(1, rows):
        pl.semaphore_signal(barrier, inc=1, device_id=(lax.rem(r + d, rows), c), device_id_type=MESH)
    for d in range(1, cols):
        pl.semaphore_signal(barrier, inc=1, device_id=(r, lax.rem(c + d, cols)), device_id_type=MESH)

    def put_factor(block, off):
        hi, lo = split(block)
        wcat[:rank, pl.ds(off, CHUNK)] = hi
        wcat[rank:, pl.ds(off, CHUNK)] = lo

    def times(k):
        at = pl.ds(pl.multiple_of(k * CHUNK, CHUNK), CHUNK)
        w = wcat[:, at]
        acc[...] += dot(w, ghi[at, :], NN) + dot(w, glo[at, :], NN)

    acc[...] = jnp.zeros_like(acc)

    @pl.loop(0, full)
    def _(k):
        slot = lax.rem(k, SLOTS)
        off = pl.multiple_of(k * CHUNK, CHUNK)
        put_factor(w0_ref[:, pl.ds(off, CHUNK)], off)
        load(k).wait()
        hi, lo = split(fbuf[slot])
        ghi[pl.ds(off, CHUNK), :] = hi
        glo[pl.ds(off, CHUNK), :] = lo

        @pl.when(k + SLOTS < full)
        def _():
            load(k + SLOTS).start()

        times(k)

    if rest:
        wcat[:, cut:] = jnp.zeros((2 * rank, CHUNK), BF16)
        ghi[cut:, :] = jnp.zeros((CHUNK, depth), BF16)
        glo[cut:, :] = jnp.zeros((CHUNK, depth), BF16)
        hi, lo = split(w0_ref[:, cut:n])
        wcat[:rank, cut:n] = hi
        wcat[rank:, cut:n] = lo
        load_tail.wait()
        hi, lo = split(ftail[...])
        ghi[cut:n, :] = hi
        glo[cut:n, :] = lo
        times(full)

    pl.semaphore_wait(barrier, rows + cols - 2)

    def copy(src, dst, ssem, rsem, dev):
        cp = pltpu.make_async_remote_copy(
            src_ref=src, dst_ref=dst, send_sem=ssem, recv_sem=rsem, device_id=dev, device_id_type=MESH
        )
        cp.start()
        return cp

    def exchange(slots, me, count, ssem, rsem, device):
        cps = []
        for d in range(1, count):
            cps.append(copy(slots.at[me], slots.at[me], ssem.at[d - 1], rsem.at[d - 1], device(lax.rem(me + d, count))))
        for cp in cps:
            cp.wait()
        total = slots[0]
        for i in range(1, count):
            total = total + slots[i]
        return total

    def rows_at(start, size):
        return pl.ds(pl.multiple_of(start, 8), size)

    bounds = [(chunks * s) // SEGMENTS for s in range(SEGMENTS + 1)]

    for step in range(ITERS):
        last = step == ITERS - 1
        if step:
            acc[...] = jnp.zeros_like(acc)
            pl.loop(0, chunks)(times)
        ypart[...] = acc[:rank, :] + acc[rank:, :]
        cps = []
        for d in range(1, cols):
            p = lax.rem(c + d, cols)
            cps.append(copy(ypart.at[rows_at(p * quarter, quarter)], yrecv.at[d - 1], ys_s.at[d - 1], ys_r.at[d - 1], (r, p)))
        for cp in cps:
            cp.wait()
        own = rows_at(c * quarter, quarter)
        total = ypart[own, :]
        for d in range(1, cols):
            total = total + yrecv[d - 1]
        yfull[own, :] = total
        cps = []
        for d in range(1, cols):
            p = lax.rem(c + d, cols)
            cps.append(copy(yfull.at[own], yfull.at[own], ya_s.at[d - 1], ya_r.at[d - 1], (r, p)))
        for cp in cps:
            cp.wait()
        grow[r] = pack(dot(yfull[...], yfull[...], NT, HIGH))
        gram = unpack(exchange(grow, r, rows, gr_s, gr_r, lambda p: (p, c)))
        _, inverse = chol_inverse(gram)
        left = dot(inverse, yfull[...], NN, HIGH)
        if last:
            left_ref[...] = left

            @pl.when(q == c)
            def _():
                lsel[y] = left
        hi, lo = split(left)
        lcat[:rank, :] = hi
        lcat[rank:, :] = lo
        gacc[...] = jnp.zeros_like(gacc)
        flight = {}
        sends = []
        pair = (r + 1 - 2 * y, c)

        def start(key, cp):
            flight.setdefault(key, []).append(cp)
            sends.append(cp)

        def arrived(key):
            for cp in flight[key]:
                cp.wait_recv()

        def seg_at(s):
            return pl.ds(bounds[s] * CHUNK, (bounds[s + 1] - bounds[s]) * CHUNK)

        def stage0(s):
            @pl.loop(bounds[s], bounds[s + 1])
            def _(k):
                at = pl.ds(pl.multiple_of(k * CHUNK, CHUNK), CHUNK)
                part = (dot(ghi[at, :], lcat[...], NT) + dot(glo[at, :], lcat[...], NT)).T
                zpart[:, at] = part[:rank] + part[rank:]

            other = rows_at((1 - y) * half, half)
            start(("p", s), copy(zpart.at[other, seg_at(s)], zpair.at[:, seg_at(s)], p_s.at[s], p_r.at[s], pair))

        def stage1(s):
            arrived(("p", s))
            at = seg_at(s)
            zpair[:, at] = zpair[:, at] + zpart[rows_at(y * half, half), at]
            for d in range(1, groups):
                p = lax.rem(q + d, groups)
                start(
                    ("q", s),
                    copy(
                        zpair.at[rows_at(p * eighth, eighth), at], zgroup.at[d - 1, :, at],
                        q_s.at[s, d - 1], q_r.at[s, d - 1], (2 * p + y, c),
                    ),
                )

        mine = rows_at(y * half + q * eighth, eighth)

        def stage2(s):
            arrived(("q", s))
            at = seg_at(s)
            total = zpair[rows_at(q * eighth, eighth), at]
            for d in range(1, groups):
                total = total + zgroup[d - 1, :, at]
            zfull[mine, at] = total
            for d in range(1, groups):
                p = lax.rem(q + d, groups)
                start(
                    ("a", s),
                    copy(zfull.at[mine, at], zfull.at[mine, at], a_s.at[s, d - 1], a_r.at[s, d - 1], (2 * p + y, c)),
                )

        def stage3(s):
            arrived(("a", s))
            at = seg_at(s)
            kept = rows_at(y * half, half)
            start(("b", s), copy(zfull.at[kept, at], zfull.at[kept, at], b_s.at[s], b_r.at[s], pair))

        def stage4(s):
            arrived(("b", s))
            block = zfull[:, seg_at(s)]
            gacc[...] += dot(block, block, NT, HIGH)

        stages = (stage0, stage1, stage2, stage3, stage4)
        for tick in range(SEGMENTS + len(stages) - 1):
            for i, stage in enumerate(stages):
                if 0 <= tick - i < SEGMENTS:
                    stage(tick - i)
        for cp in sends:
            cp.wait_send()
        if last:
            def spread(d):
                return pltpu.make_async_remote_copy(
                    src_ref=left_ref, dst_ref=lsel.at[y], send_sem=l_s.at[d - 1], recv_sem=l_r.at[0],
                    device_id=(2 * lax.rem(q + d, groups) + y, c), device_id_type=MESH,
                )

            @pl.when(q == c)
            def _():
                for d in range(1, groups):
                    spread(d).start()
        gcol[c] = pack(gacc[...])
        gram = unpack(exchange(gcol, c, cols, gc_s, gc_r, lambda p: (r, p)))
        upper, inverse = chol_inverse(gram)
        if not last:

            @pl.loop(0, chunks)
            def _(k):
                off = pl.multiple_of(k * CHUNK, CHUNK)
                put_factor(dot(inverse, zfull[:, pl.ds(off, CHUNK)], NN, HIGH), off)

    @pl.when(q != c)
    def _():
        spread(1).wait_recv()

    swap = copy(lsel.at[y], lsel.at[y], m_s.at[0], m_r.at[0], pair)
    gacc[...] = jnp.zeros_like(gacc)

    @pl.loop(0, full)
    def _(k):
        at = pl.ds(pl.multiple_of(k * CHUNK, CHUNK), CHUNK)
        block = dot(inverse, zfull[:, at], NN, HIGH)
        right_ref[:, at] = block
        gacc[...] += dot(act_ref[:, at], block, NT, HIGH)

    if rest:
        block = dot(inverse, zfull[:, cut:], NN, HIGH)[:, :rest]
        right_ref[:, cut:n] = block
        gacc[...] += dot(act_ref[:, cut:n], block, NT, HIGH)
    swap.wait()

    @pl.when(q == c)
    def _():
        for d in range(1, groups):
            spread(d).wait_send()

    token_left = dot(og_ref[:, :depth], lsel[0], NT, HIGH) + dot(og_ref[:, depth:], lsel[1], NT, HIGH)
    tok[c] = jnp.concatenate([token_left, gacc[...]], axis=1)
    tokens = exchange(tok, c, cols, t_s, t_r, lambda p: (r, p))
    mixed = dot(tokens[:, :rank], upper, NT, HIGH)
    score_ref[...] = dot(jnp.ones((8, rank), F32), mixed * tokens[:, rank:], NT, HIGH)


def iterate(gradient, start, activations, out_grads, rows, cols):
    n, depth = gradient.shape
    rank = start.shape[0]
    tokens = activations.shape[0]
    wide = -(-n // CHUNK) * CHUNK
    dma = pltpu.SemaphoreType.DMA
    groups = rows // 2
    vmem = pl.BlockSpec(memory_space=pltpu.VMEM)
    return pl.pallas_call(
        functools.partial(kernel, rows, cols),
        out_shape=(
            jax.ShapeDtypeStruct((rank, depth), F32),
            jax.ShapeDtypeStruct((rank, n), F32),
            jax.ShapeDtypeStruct((8, tokens), F32),
        ),
        in_specs=[pl.BlockSpec(memory_space=pl.ANY), vmem, vmem, vmem],
        out_specs=(vmem, vmem, vmem),
        scratch_shapes=[
            pltpu.VMEM((wide, depth), BF16),
            pltpu.VMEM((wide, depth), BF16),
            pltpu.VMEM((SLOTS, CHUNK, depth), F32),
            pltpu.VMEM((n % CHUNK or 8, depth), F32),
            pltpu.VMEM((2 * rank, wide), BF16),
            pltpu.VMEM((2 * rank, depth), BF16),
            pltpu.VMEM((2 * rank, depth), F32),
            pltpu.VMEM((rank, depth), F32),
            pltpu.VMEM((cols - 1, rank // cols, depth), F32),
            pltpu.VMEM((rank, depth), F32),
            pltpu.VMEM((rank, wide), F32),
            pltpu.VMEM((rank // 2, wide), F32),
            pltpu.VMEM((groups - 1, rank // rows, wide), F32),
            pltpu.VMEM((rank, wide), F32),
            pltpu.VMEM((rank, rank), F32),
            pltpu.VMEM((rows, rank // 2, 2 * rank), F32),
            pltpu.VMEM((cols, rank // 2, 2 * rank), F32),
            pltpu.VMEM((2, rank, depth), F32),
            pltpu.VMEM((cols, tokens, 2 * rank), F32),
            dma((SLOTS,)), dma((1,)),
            dma((cols - 1,)), dma((cols - 1,)), dma((cols - 1,)), dma((cols - 1,)),
            dma((rows - 1,)), dma((rows - 1,)), dma((cols - 1,)), dma((cols - 1,)),
            dma((SEGMENTS,)), dma((SEGMENTS,)),
            dma((SEGMENTS, groups - 1)), dma((SEGMENTS, groups - 1)),
            dma((SEGMENTS, groups - 1)), dma((SEGMENTS, groups - 1)),
            dma((SEGMENTS,)), dma((SEGMENTS,)),
            dma((groups - 1,)), dma((1,)), dma((1,)), dma((1,)), dma((cols - 1,)), dma((cols - 1,)),
        ],
        compiler_params=pltpu.CompilerParams(
            collective_id=0, has_side_effects=True, vmem_limit_bytes=63 * 1024 * 1024
        ),
        cost_estimate=pl.CostEstimate(flops=16 * depth * n * rank, bytes_accessed=4 * depth * n, transcendentals=0),
    )(gradient, start, activations, out_grads)


def factor_with(block, gram):
    lower = jnp.linalg.cholesky(gram)
    return (
        lax.linalg.triangular_solve(lower, block, left_side=False, lower=True, transpose_a=True),
        lower,
    )


def full_dot(a, b):
    return jnp.dot(a, b, precision=HIGH, preferred_element_type=F32)


def iterate_plain(gradient, start_block):
    omega = start_block
    for step in range(ITERS):
        ysum = lax.psum(full_dot(gradient, omega), "cols")
        left, lower_y = factor_with(ysum, lax.psum(full_dot(ysum.T, ysum), "rows"))
        zsum = lax.psum(full_dot(gradient.T, left), "rows")
        right, lower_z = factor_with(zsum, lax.psum(full_dot(zsum.T, zsum), "cols"))
        omega = right
    return left, right, lower_z


def fits(rows, cols, depth, n, rank, tokens, grad_cols):
    wide = -(-n // CHUNK) * CHUNK
    held = 4 * depth * wide + 4 * rank * wide * 7
    return (
        rows == 2 * cols and cols > 1 and rank % (8 * rows) == 0 and 2 * rank == 128 and depth % 128 == 0
        and n % 16 == 0 and n // CHUNK >= max(SEGMENTS, SLOTS) and held < 50 * 1024 * 1024
        and grad_cols == 2 * depth and tokens % 8 == 0 and tokens <= 128
    )


def per_device(rows, cols, gradient, start_block, activations, out_grads):
    depth, n = gradient.shape
    rank = start_block.shape[1]
    tokens, grad_cols = out_grads.shape
    if fits(rows, cols, depth, n, rank, tokens, grad_cols):
        left, right, scores = iterate(gradient.T, start_block.T, activations, out_grads, rows, cols)
        return left.T, right.T, scores[0]
    left, right, lower_z = iterate_plain(gradient, start_block)
    whole_rows = lax.all_gather(left, "rows", axis=0, tiled=True)
    left_cols = lax.dynamic_slice_in_dim(whole_rows, lax.axis_index("cols") * grad_cols, grad_cols, 0)
    token_left, token_right = lax.psum((full_dot(out_grads, left_cols), full_dot(activations, right)), "cols")
    scores = jnp.sum(full_dot(token_left, lower_z) * token_right, axis=1)
    return (left, right, scores)


def solution(mesh):
    placed = (P("rows", "cols"), P("cols", None), P("rows", "cols"), P("rows", "cols"))
    return jax.shard_map(
        functools.partial(per_device, mesh.shape["rows"], mesh.shape["cols"]),
        mesh=mesh,
        in_specs=placed,
        out_specs=(P("rows", None), P("cols", None), P("rows")),
        check_vma=False,
    )
```
